768 devices in a mesh: rep: 192 (over z, y, core), fsdp: 4 (over x).
Axes of the slice: x: 4, y: 8, z: 12, core: 2. Of those that a mesh axis runs over, the one named last changes fastest.
Arguments:
- activations: bfloat16 [98304, 8192], P(('rep', 'fsdp')), may hold values from -7.153361557201429 to 7.153361557201429
- upstream: bfloat16 [98304, 512], P(('rep', 'fsdp')), may hold values from -0.3161369 to 0.3161369
- q_start: float32 [4, 4, 512], P('fsdp'), may hold values from -6 to 6
Outputs:
- error_feedback: bfloat16 [192, 8192, 512], P('rep', 'fsdp')
- p_basis: float32 [4, 4, 2048], P('fsdp')
- q_factor: float32 [4, 4, 512], P('fsdp')
The draws below stay inside these ranges and needn't reach their ends.
All inputs are finite; a program needn't handle non-finite values.
Results may differ from the reference program's by a relative error of at most 0.015.
Values may be sent and summed in bfloat16 or wider, within the bound.
No kernel may reach another device: no remote copies, remote signals or barrier semaphores. Data moves between devices by JAX's collectives and lax.ppermute only.
A program may use at most 64 MiB of HBM per device.

```python
import jax
import jax.numpy as jnp
from jax import lax

D = 8192
KVW = 512
RANK = 4
TOK_DEV = 128
GROUP_TOKENS = 512
TOKENS = 98304
N_REP = 192
N_FSDP = 4


def unit_values(key, shape):
    return jnp.clip(jax.random.normal(key, shape, jnp.float32), -3.0, 3.0)


def noise_values(key, shape):
    return jnp.clip(jax.random.normal(key, shape, jnp.float32), -4.0, 4.0)


def shared_parts(key):
    strength = jnp.array([1.2, 1.0, 0.8, 0.6, 0.4], jnp.float32)
    tok_scale = GROUP_TOKENS ** (-0.25)
    weights = jnp.sqrt(strength) * tok_scale
    token_signs = jax.random.rademacher(jax.random.fold_in(key, 101), (TOKENS, 5), dtype=jnp.float32)
    left_dirs = unit_values(jax.random.fold_in(key, 102), (5, D))
    right_dirs = unit_values(jax.random.fold_in(key, 103), (5, KVW))
    return (token_signs * weights[None, :], left_dirs, right_dirs)


def draw_activations(key, part):
    coeffs, left_dirs, right_dirs = shared_parts(key)
    noise_part = noise_values(jax.random.fold_in(key, 104), (TOKENS, D))
    common = jnp.dot(coeffs, left_dirs, precision=lax.Precision.HIGHEST)
    return (noise_part + common).astype(jnp.bfloat16)


def draw_upstream(key, part):
    coeffs, left_dirs, right_dirs = shared_parts(key)
    noise_part = noise_values(jax.random.fold_in(key, 105), (TOKENS, KVW))
    common = jnp.dot(coeffs, right_dirs, precision=lax.Precision.HIGHEST)
    return ((noise_part + common) * GROUP_TOKENS ** (-0.5)).astype(jnp.bfloat16)


def block_levels(key, extent, cuts, least, high):
    def one(axis_at, shards_of):
        draws = jax.random.uniform(jax.random.fold_in(jax.random.fold_in(key, 6), axis_at), (shards_of,), jnp.float32, least / len(cuts), high / len(cuts))
        return jnp.repeat(jnp.exp(draws), extent[axis_at] // shards_of).reshape((-1,) + (1,) * (len(extent) - axis_at - 1))

    gain = one(*cuts[0])
    for cut in cuts[1:]:
        gain = gain * one(*cut)
    return gain


def noise(own_key, shape, deviation, limit, cuts=(), kind=jnp.bfloat16):
    values = deviation * jax.random.normal(own_key, shape, jnp.float32)
    if cuts:
        values = values * block_levels(own_key, shape, cuts, -0.22, 0.18)
    return jnp.clip(values, -limit, limit).astype(kind)


def setup_inputs(seed: int = 0) -> dict:
    streams_of = jax.random.split(jax.random.key(seed), 4)
    return {
        "activations": draw_activations(jax.random.fold_in(streams_of[3], 71), 0),
        "upstream": draw_upstream(jax.random.fold_in(streams_of[3], 71), 0),
        "q_start": noise(streams_of[2], (N_FSDP, RANK, KVW), 1.0, 6.0, ((0, 4),), jnp.float32),
    }


def replica_grad(xs, us):
    total = jnp.zeros((D, KVW), jnp.float32)
    for fidx in range(N_FSDP):
        part = jnp.dot(xs[fidx].T, us[fidx], preferred_element_type=jnp.float32).astype(jnp.bfloat16)
        part = lax.optimization_barrier(part)
        total = total + part.astype(jnp.float32)
    return total.reshape(N_FSDP, D // N_FSDP, KVW)

def orthonormal(rows_in):
    basis = []
    for i in range(RANK):
        vec = rows_in[i]
        for prev in basis:
            vec = vec - jnp.sum(vec * prev) * prev
        basis.append(vec / jnp.sqrt(jnp.sum(vec * vec) + 1e-06))
    return jnp.stack(basis)

def reference(activations, upstream, q_start):
    acts = activations.reshape(N_REP, N_FSDP, TOK_DEV, D)
    cots = upstream.reshape(N_REP, N_FSDP, TOK_DEV, KVW)
    high = lax.Precision.HIGHEST

    def left_step(carry, pair):
        mats = replica_grad(pair[0], pair[1])
        return (carry + jnp.einsum('frk,fnk->frn', q_start, mats, precision=high), None)
    p_sum, _ = lax.scan(left_step, jnp.zeros((N_FSDP, RANK, D // N_FSDP), jnp.float32), (acts, cots))
    p_basis = jax.vmap(orthonormal)(p_sum)

    def right_step(carry, pair):
        mats = replica_grad(pair[0], pair[1])
        return (carry + jnp.einsum('frn,fnk->frk', p_basis, mats, precision=high), None)
    q_factor, _ = lax.scan(right_step, jnp.zeros((N_FSDP, RANK, KVW), jnp.float32), (acts, cots))
    approx = jnp.einsum('frn,frk->fnk', p_basis, q_factor / N_REP, precision=high)

    def residual(pair):
        mats = replica_grad(pair[0], pair[1])
        return (mats - approx).astype(jnp.bfloat16).reshape(D, KVW)
    error_feedback = lax.map(residual, (acts, cots))
    return (error_feedback, p_basis, q_factor)
```

```python
import jax
import jax.numpy as jnp
from jax import lax
from jax.experimental import pallas as pl
from jax.experimental.pallas import tpu as pltpu
from jax.sharding import Mesh
from jax.sharding import PartitionSpec as P

REP = ("rep_0", "rep_1", "rep_2")
REP_FSDP = ("rep_0", "rep_1", "rep_2", "fsdp")
VMEM = pl.BlockSpec(memory_space=pltpu.VMEM)
NN = (((1,), (0,)), ((), ()))
NT = (((1,), (1,)), ((), ()))
F32 = jnp.float32
BF16 = jnp.bfloat16


def exchange(array, axis):
    return lax.all_to_all(array, axis, 0, 0, tiled=True)


def sent_to_all(array, axis):
    return exchange(jnp.broadcast_to(array[None], (lax.axis_size(axis), *array.shape)), axis)


def pieces(value):
    first = value.astype(BF16)
    rest = value - first.astype(F32)
    second = rest.astype(BF16)
    third = (rest - second.astype(F32)).astype(BF16)
    return first, second, third


def exact_dot(value, short, dims):
    rows = value.shape[0]
    stacked = jnp.concatenate([p.astype(F32) for p in pieces(value)], axis=0).astype(BF16)
    out = lax.dot_general(stacked, short, dims, preferred_element_type=F32)
    return out[:rows] + (out[rows : 2 * rows] + out[2 * rows :])


def turn_kernel(me_ref, act_ref, up_ref, *refs):
    del me_ref
    groups = len(refs) - 2
    out_refs, held_ref, sems = refs[:groups], refs[-2], refs[-1]
    rows = act_ref.shape[1]
    step = pl.program_id(0)
    held_ref[step, :rows] = act_ref[...].T
    held_ref[step, rows:] = up_ref[...].T
    for k in range(groups):
        copy = pltpu.make_async_copy(held_ref.at[k], out_refs[k], sems.at[k])
        pl.when(step == k)(copy.start)
        pl.when(step == groups - 1)(copy.wait)


def turned(me, activations, upstream, groups):
    tok, width = activations.shape
    rows, cols = width // groups, upstream.shape[1]
    chunk = jax.ShapeDtypeStruct((rows + cols, tok), BF16)
    return pl.pallas_call(
        turn_kernel,
        grid_spec=pltpu.PrefetchScalarGridSpec(
            num_scalar_prefetch=1,
            grid=(groups,),
            in_specs=[
                pl.BlockSpec((tok, rows), lambda k, me_ref: (0, lax.rem(me_ref[0] + k, groups))),
                pl.BlockSpec((tok, cols), lambda k, me_ref: (0, 0)),
            ],
            out_specs=[pl.BlockSpec(memory_space=pl.ANY)] * groups,
            scratch_shapes=[
                pltpu.VMEM((groups, rows + cols, tok), BF16),
                pltpu.SemaphoreType.DMA((groups,)),
            ],
        ),
        out_shape=[chunk] * groups,
        name="turn",
    )(me, activations, upstream)


def left_kernel(me_ref, q_ref, *refs):
    chunk_refs, out_ref = refs[:-1], refs[-1]
    blocks, groups, rank, size = out_ref.shape
    rows = blocks * size
    ups = chunk_refs[0][rows:]
    for k in range(groups):
        g = lax.rem(me_ref[0] + k, groups)
        weights = exact_dot(q_ref[g], ups, NN)
        left = exact_dot(weights, chunk_refs[k][:rows], NT)
        for b in range(blocks):
            out_ref[b, g] = left[:, b * size : (b + 1) * size]


def left_parts(me, q_all, chunks, blocks):
    groups, rank, cols = q_all.shape
    rows = chunks[0].shape[0] - cols
    return pl.pallas_call(
        left_kernel,
        in_specs=[pl.BlockSpec(memory_space=pltpu.SMEM)] + [VMEM] * (groups + 1),
        out_specs=VMEM,
        out_shape=jax.ShapeDtypeStruct((blocks, groups, rank, rows // blocks), F32),
        name="left",
    )(me, q_all, *chunks)


def right_kernel(p_ref, *refs):
    chunk_refs, basis_ref, right_ref = refs[:-2], refs[-2], refs[-1]
    blocks, rank, size = p_ref.shape
    rows = blocks * size
    basis = []
    for i in range(rank):
        vec = p_ref[:, i, :]
        for prev in basis:
            vec = vec - jnp.sum(vec * prev, keepdims=True) * prev
        vec = vec / jnp.sqrt(jnp.sum(vec * vec, keepdims=True) + 1e-06)
        basis.append(vec)
        for b in range(blocks):
            basis_ref[i : i + 1, b * size : (b + 1) * size] = vec[b : b + 1]
    whole = basis_ref[...]
    total = jnp.zeros(right_ref.shape, F32)
    for chunk_ref in chunk_refs:
        weights = exact_dot(whole, chunk_ref[:rows], NN)
        total = total + exact_dot(weights, chunk_ref[rows:], NT)
    right_ref[...] = total


def basis_and_right(p_blocks, chunks):
    blocks, rank, size = p_blocks.shape
    rows = blocks * size
    return pl.pallas_call(
        right_kernel,
        in_specs=[VMEM] * (1 + len(chunks)),
        out_specs=[VMEM] * 2,
        out_shape=[
            jax.ShapeDtypeStruct((rank, rows), F32),
            jax.ShapeDtypeStruct((rank, chunks[0].shape[0] - rows), F32),
        ],
        name="right",
    )(p_blocks, *chunks)


def last_kernel(scale, parts_ref, basis_ref, *refs):
    groups = len(refs) // 2 - 1
    chunk_refs, up_refs = refs[:groups], refs[groups : 2 * groups]
    error_ref, factor_ref = refs[2 * groups :]
    factor = parts_ref[0]
    for part in range(1, parts_ref.shape[0]):
        factor = factor + parts_ref[part]
    factor_ref[...] = factor
    acts = jnp.concatenate([ref[...] for ref in chunk_refs], axis=1)
    ups = jnp.concatenate([ref[...] for ref in up_refs], axis=1)
    grad = lax.dot_general(acts, ups, NT, preferred_element_type=F32)
    b0, b1, b2 = (p.astype(F32) for p in pieces(basis_ref[...]))
    q0, q1, q2 = (p.astype(F32) for p in pieces(factor * scale))
    lefts = jnp.concatenate([b0, b0, b1, b0, b1, b2], axis=0).astype(BF16)
    rights = jnp.concatenate([q0, q1, q0, q2, q1, q0], axis=0).astype(BF16)
    approx = lax.dot_general(lefts, rights, (((0,), (0,)), ((), ())), preferred_element_type=F32)
    error_ref[...] = (grad - approx).astype(BF16)


def error_and_factor(parts, basis, chunks, replicas):
    groups = len(chunks)
    height, tok = chunks[0].shape
    rank, rows = basis.shape
    cols = height - rows
    steps = 4
    step_rows = rows // steps

    def kernel(*refs):
        last_kernel(1.0 / replicas, *refs)

    return pl.pallas_call(
        kernel,
        grid=(steps,),
        in_specs=[
            pl.BlockSpec(parts.shape, lambda s: (0, 0, 0)),
            pl.BlockSpec((rank, step_rows), lambda s: (0, s)),
        ]
        + [pl.BlockSpec((step_rows, tok), lambda s: (s, 0))] * groups
        + [pl.BlockSpec((cols, tok), lambda s: (rows // cols, 0))] * groups,
        out_specs=[
            pl.BlockSpec((step_rows, cols), lambda s: (s, 0)),
            pl.BlockSpec((rank, cols), lambda s: (0, 0)),
        ],
        out_shape=[
            jax.ShapeDtypeStruct((rows, cols), BF16),
            jax.ShapeDtypeStruct((rank, cols), F32),
        ],
        name="last",
    )(parts, basis, *chunks, *chunks)


def on_device(activations, upstream, q_start):
    groups = lax.axis_size("fsdp")
    replicas = lax.axis_size(REP)
    pairs = ("rep_1", "rep_2")
    blocks = lax.axis_size(pairs)
    rank = q_start.shape[1]
    me = lax.axis_index("fsdp")[None]
    q_all = sent_to_all(q_start[0], "fsdp")
    chunks = turned(me, activations, upstream, groups)
    parts = left_parts(me, q_all, chunks, blocks)
    size = parts.shape[-1]
    parts = exchange(parts.reshape(blocks * groups, rank, size), ("rep_1", "rep_2", "fsdp"))
    parts, sent = lax.optimization_barrier((parts, chunks[1:]))
    chunks = [chunks[0]] + [
        lax.ppermute(chunk, "fsdp", [(i, (i + k + 1) % groups) for i in range(groups)])
        for k, chunk in enumerate(sent)
    ]
    mine = jnp.sum(parts, axis=0)
    mine = jnp.sum(sent_to_all(mine, "rep_0"), axis=0)
    p_blocks = sent_to_all(mine, pairs)
    p_basis, right = basis_and_right(p_blocks, chunks)
    right = jnp.sum(sent_to_all(right, "rep_0"), axis=0)
    right_parts = sent_to_all(right, pairs)
    error_feedback, q_factor = error_and_factor(right_parts, p_basis, chunks, replicas)
    return (error_feedback[None], p_basis[None], q_factor[None])


def solution(mesh):
    split = Mesh(
        mesh.devices.reshape(12, 8, 2, mesh.shape["fsdp"]), ("rep_0", "rep_1", "rep_2", "fsdp")
    )
    return jax.shard_map(
        on_device,
        mesh=split,
        in_specs=(P(REP_FSDP, None), P(REP_FSDP, None), P("fsdp", None, None)),
        out_specs=(P(REP, "fsdp", None), P("fsdp", None, None), P("fsdp", None, None)),
        check_vma=False,
    )
```

```python
import jax
import jax.numpy as jnp
from jax import lax
from jax.experimental import pallas as pl
from jax.experimental.pallas import tpu as pltpu
from jax.sharding import Mesh
from jax.sharding import PartitionSpec as P

REP = ("rep_0", "rep_1", "rep_2")
REP_FSDP = ("rep_0", "rep_1", "rep_2", "fsdp")
VMEM = pl.BlockSpec(memory_space=pltpu.VMEM)
NN = (((1,), (0,)), ((), ()))
NT = (((1,), (1,)), ((), ()))
TN = (((0,), (0,)), ((), ()))
F32 = jnp.float32
BF16 = jnp.bfloat16


def exchange(array, axis):
    return lax.all_to_all(array, axis, 0, 0, tiled=True)


def sent_to_all(array, axis):
    return exchange(jnp.broadcast_to(array[None], (lax.axis_size(axis), *array.shape)), axis)


def pieces(value):
    first = value.astype(BF16)
    rest = value - first.astype(F32)
    second = rest.astype(BF16)
    third = (rest - second.astype(F32)).astype(BF16)
    return first, second, third


def exact_dot(value, short, dims):
    rows = value.shape[0]
    stacked = jnp.concatenate([p.astype(F32) for p in pieces(value)], axis=0).astype(BF16)
    out = lax.dot_general(stacked, short, dims, preferred_element_type=F32)
    return out[:rows] + (out[rows : 2 * rows] + out[2 * rows :])


def in_vmem(shape, dtype=F32):
    return pltpu.VMEM(shape, dtype)


def held(*arrays):
    return [pltpu.with_memory_space_constraint(array, pltpu.VMEM) for array in arrays]


def repeat_kernel(value_ref, out_ref):
    for k in range(out_ref.shape[0]):
        out_ref[k] = value_ref[...]


def repeated(value, times):
    return pl.pallas_call(
        repeat_kernel,
        in_specs=[VMEM],
        out_specs=VMEM,
        out_shape=in_vmem((times, *value.shape)),
        name="repeat",
    )(value)


def pack_kernel(me_ref, act_ref, up_ref, *refs):
    chunk_refs, sems = refs[:-1], refs[-1]
    groups = len(chunk_refs)
    rows = act_ref.shape[1] // groups
    copies = []
    for k, chunk_ref in enumerate(chunk_refs):
        start = pl.multiple_of(lax.rem(me_ref[0] + k, groups) * rows, rows)
        pairs = (
            (act_ref.at[:, pl.ds(start, rows)], chunk_ref.at[:, :rows]),
            (up_ref, chunk_ref.at[:, rows:]),
        )
        for i, (source, target) in enumerate(pairs):
            copies.append(pltpu.make_async_copy(source, target, sems.at[2 * k + i]))
    for copy in copies:
        copy.start()
    for copy in copies:
        copy.wait()


def packed(me, activations, upstream, groups):
    tok, width = activations.shape
    chunk = in_vmem((tok, width // groups + upstream.shape[1]), BF16)
    return pl.pallas_call(
        pack_kernel,
        in_specs=[pl.BlockSpec(memory_space=pltpu.SMEM)] + [pl.BlockSpec(memory_space=pl.ANY)] * 2,
        out_specs=[VMEM] * groups,
        out_shape=[chunk] * groups,
        scratch_shapes=[pltpu.SemaphoreType.DMA((2 * groups,))],
        name="pack",
    )(me, activations, upstream)


def left_kernel(me_ref, q_ref, *refs):
    chunk_refs, out_ref = refs[:-1], refs[-1]
    blocks, groups, rank, size = out_ref.shape
    rows = blocks * size
    ups = chunk_refs[0][:, rows:]
    for k in range(groups):
        g = lax.rem(me_ref[0] + k, groups)
        weights = exact_dot(q_ref[g], ups, NT)
        left = exact_dot(weights, chunk_refs[k][:, :rows], NN)
        for b in range(blocks):
            out_ref[b, g] = left[:, b * size : (b + 1) * size]


def left_parts(me, q_all, chunks, blocks):
    groups, rank, cols = q_all.shape
    rows = chunks[0].shape[1] - cols
    return pl.pallas_call(
        left_kernel,
        in_specs=[pl.BlockSpec(memory_space=pltpu.SMEM)] + [VMEM] * (groups + 1),
        out_specs=VMEM,
        out_shape=in_vmem((blocks, groups, rank, rows // blocks)),
        name="left",
    )(me, *held(q_all, *chunks))


def right_kernel(p_ref, *refs):
    chunk_refs, basis_ref, out_ref = refs[:-2], refs[-2], refs[-1]
    blocks, groups, rank, size = p_ref.shape
    rows = blocks * size
    basis = []
    for i in range(rank):
        vec = p_ref[:, 0, i, :]
        for g in range(1, groups):
            vec = vec + p_ref[:, g, i, :]
        for prev in basis:
            vec = vec - jnp.sum(vec * prev, keepdims=True) * prev
        vec = vec / jnp.sqrt(jnp.sum(vec * vec, keepdims=True) + 1e-06)
        basis.append(vec)
        for b in range(blocks):
            basis_ref[i : i + 1, b * size : (b + 1) * size] = vec[b : b + 1]
    whole = basis_ref[...]
    total = jnp.zeros(out_ref.shape[1:], F32)
    for chunk_ref in chunk_refs:
        weights = exact_dot(whole, chunk_ref[:, :rows], NT)
        total = total + exact_dot(weights, chunk_ref[:, rows:], NN)
    for k in range(out_ref.shape[0]):
        out_ref[k] = total


def basis_and_right(p_parts, chunks, copies):
    blocks, groups, rank, size = p_parts.shape
    rows = blocks * size
    return pl.pallas_call(
        right_kernel,
        in_specs=[VMEM] * (1 + groups),
        out_specs=[VMEM] * 2,
        out_shape=[
            in_vmem((rank, rows)),
            in_vmem((copies, rank, chunks[0].shape[1] - rows)),
        ],
        name="right",
    )(*held(p_parts, *chunks))


def error_and_factor(parts, basis, chunks, replicas):
    groups = len(chunks)
    rank, rows = basis.shape
    cols = chunks[0].shape[1] - rows
    steps = 4
    step_rows = rows // steps
    scale = 1.0 / replicas

    def kernel(parts_ref, basis_ref, *refs):
        chunk_refs = refs[:groups]
        error_ref, factor_ref, held_ref, sems = refs[groups:]
        factor = parts_ref[0]
        for part in range(1, parts_ref.shape[0]):
            factor = factor + parts_ref[part]
        factor_ref[...] = factor
        q0, q1, q2 = (p.astype(F32) for p in pieces(factor * scale))
        rights = jnp.concatenate([q0, q1, q0, q2, q1, q0], axis=0).astype(BF16)
        ups = jnp.concatenate([ref[:, rows:] for ref in chunk_refs], axis=0)
        copies = []
        for step in range(steps):
            span = slice(step * step_rows, (step + 1) * step_rows)
            acts = jnp.concatenate([ref[:, span] for ref in chunk_refs], axis=0)
            grad = lax.dot_general(acts, ups, TN, preferred_element_type=F32)
            b0, b1, b2 = (p.astype(F32) for p in pieces(basis_ref[:, span]))
            lefts = jnp.concatenate([b0, b0, b1, b0, b1, b2], axis=0).astype(BF16)
            approx = lax.dot_general(lefts, rights, TN, preferred_element_type=F32)
            held_ref[span] = (grad - approx).astype(BF16)
            copy = pltpu.make_async_copy(held_ref.at[span], error_ref.at[span], sems.at[step])
            copy.start()
            copies.append(copy)
        for copy in copies:
            copy.wait()

    return pl.pallas_call(
        kernel,
        in_specs=[VMEM] * (2 + groups),
        out_specs=[pl.BlockSpec(memory_space=pl.ANY), VMEM],
        out_shape=[
            jax.ShapeDtypeStruct((rows, cols), BF16),
            jax.ShapeDtypeStruct((rank, cols), F32),
        ],
        scratch_shapes=[
            pltpu.VMEM((rows, cols), BF16),
            pltpu.SemaphoreType.DMA((steps,)),
        ],
        name="last",
    )(*held(parts, basis, *chunks))


def on_device(activations, upstream, q_start):
    groups = lax.axis_size("fsdp")
    replicas = lax.axis_size(REP)
    planes = lax.axis_size("rep_0")
    pairs = ("rep_1", "rep_2")
    blocks = lax.axis_size(pairs)
    me = lax.axis_index("fsdp")[None]
    q_all = exchange(repeated(q_start[0], groups), "fsdp")
    chunks = packed(me, activations, upstream, groups)
    received = [chunks[0]] + [
        lax.ppermute(chunks[k], "fsdp", [(i, (i + k) % groups) for i in range(groups)])
        for k in range(1, groups)
    ]
    parts = exchange(left_parts(me, q_all, chunks, blocks), pairs)
    parts = sent_to_all(jnp.sum(parts, axis=0), "rep_0")
    parts = jnp.sum(parts, axis=0)
    parts = jnp.broadcast_to(parts[None], (blocks, *parts.shape))
    parts = exchange(parts.reshape(blocks * groups, *parts.shape[2:]), ("rep_1", "rep_2", "fsdp"))
    parts = parts.reshape(blocks, groups, *parts.shape[1:])
    p_basis, right = basis_and_right(parts, received, planes)
    right = jnp.sum(exchange(right, "rep_0"), axis=0)
    right_parts = sent_to_all(right, pairs)
    error_feedback, q_factor = error_and_factor(right_parts, p_basis, received, replicas)
    return (error_feedback[None], p_basis[None], q_factor[None])


def solution(mesh):
    split = Mesh(
        mesh.devices.reshape(12, 8, 2, mesh.shape["fsdp"]), ("rep_0", "rep_1", "rep_2", "fsdp")
    )
    return jax.shard_map(
        on_device,
        mesh=split,
        in_specs=(P(REP_FSDP, None), P(REP_FSDP, None), P("fsdp", None, None)),
        out_specs=(P(REP, "fsdp", None), P("fsdp", None, None), P("fsdp", None, None)),
        check_vma=False,
    )
```
